32 devices in a mesh: batch: 16 (over z, y, core), seq: 2 (over x).
Axes of the slice: x: 2, y: 2, z: 4, core: 2. Of those that a mesh axis runs over, the one named last changes fastest.
Arguments:
- hidden_in: bfloat16 [16, 1024, 768], P('batch', 'seq'), may hold values from -6 to 6
- segment_ids: int32 [16, 1024], P('batch'), may hold values from 0 to 3, never falling along the last dimension, each value on 1 to 512 neighbouring positions
- qkv_weight: bfloat16 [768, 2304], replicated, may hold values from -0.3125 to 0.3125
- qv_bias: float32 [2, 768], replicated, may hold values from -5 to 5
- out_weight: bfloat16 [768, 768], replicated, may hold values from -0.4375 to 0.4375
- out_bias: float32 [768], replicated, may hold values from -3 to 3
- norm_gain: float32 [2, 768], replicated, may hold values from 0.5 to 1.5
- norm_shift: float32 [2, 768], replicated, may hold values from -3 to 3
- ffn_in_weight: bfloat16 [768, 3072], replicated, may hold values from -0.21875 to 0.21875
- ffn_in_bias: float32 [3072], replicated, may hold values from -3 to 3
- ffn_out_weight: bfloat16 [3072, 768], replicated, may hold values from -0.15625 to 0.15625
- ffn_out_bias: float32 [768], replicated, may hold values from -3 to 3
- out_grad: bfloat16 [16, 1024, 768], P('batch', 'seq'), may hold values from -6 to 6
Outputs:
- hidden_out: bfloat16 [16, 1024, 768], P('batch', 'seq')
- input_grad: bfloat16 [16, 1024, 768], P('batch', 'seq')
- grad_qkv_weight: float32 [768, 2304], replicated
- grad_qv_bias: float32 [2, 768], replicated
- grad_out_weight: float32 [768, 768], replicated
- grad_out_bias: float32 [768], replicated
- grad_norm_gain: float32 [2, 768], replicated
- grad_norm_shift: float32 [2, 768], replicated
- grad_ffn_in_weight: float32 [768, 3072], replicated
- grad_ffn_in_bias: float32 [3072], replicated
- grad_ffn_out_weight: float32 [3072, 768], replicated
- grad_ffn_out_bias: float32 [768], replicated
The draws below stay inside these ranges and needn't reach their ends.
Inputs may be any that keep to these rules, and one draw needn't show every extreme that they name: `segment_ids`: within a row the segment numbers never fall; a token attends only to tokens of its own row that carry its own number.
All inputs are finite; a program needn't handle non-finite values.
Results may differ from the reference program's by a relative error of at most 0.03.
Values may be sent and summed in bfloat16 or wider, within the bound.
A program may use at most 256 MiB of HBM per device.

```python
import math
import jax
import jax.numpy as jnp
import numpy as np
from jax import lax

D = 768
HEAD_DIM = 64
FF = 3072
SEQ_LEN = 1024
LAYERS = 2
SEGS = 4
SEG_MOST = 512
ROWS = 16


def level_of(own_key, shape, cuts, smallest, largest):
    def one(position, blocks):
        heights = jax.random.uniform(jax.random.fold_in(jax.random.fold_in(own_key, 6), position), (blocks,), jnp.float32, smallest / len(cuts), largest / len(cuts))
        return jnp.repeat(jnp.exp(heights), shape[position] // blocks).reshape((-1,) + (1,) * (len(shape) - position - 1))

    level = one(*cuts[0])
    for cut in cuts[1:]:
        level = level * one(*cut)
    return level


def split_up(amount, total, most, slope):
    loads = [(1 << 20) // math.isqrt(standing ** slope) + 1 for standing in range(2, amount + 1)]
    rest, given = total - most - (amount - 1), [1] * (amount - 1)
    while rest > 0:
        candidates = [i for i in range(amount - 1) if given[i] < most]
        mass, budget = sum([loads[i] for i in candidates]), rest
        for i in candidates:
            addition = min(most - given[i], max(1, budget * loads[i] // mass), rest)
            given[i] = given[i] + addition
            rest = rest - addition
    return np.array([most] + given)


def ragged(stream_key, amount, total, reach, skew):
    if amount == 2:
        one = jax.random.randint(stream_key, (), max(1, total - reach), min(reach, total - 1) + 1)
        return jnp.stack([one, total - one])
    lengths = jnp.asarray(split_up(amount, total, reach, skew), jnp.int32)
    pairs = (amount - 1) // 2
    donor, receiver = lengths[1:1 + 2 * pairs:2], lengths[2:2 + 2 * pairs:2]
    room = jnp.minimum(donor - 1, reach - receiver)
    moved = jax.random.randint(jax.random.fold_in(stream_key, 1), (pairs,), 0, 1 << 20) % (room + 1)
    lengths = lengths.at[1:1 + 2 * pairs:2].set(donor - moved).at[2:2 + 2 * pairs:2].set(receiver + moved)
    return lengths[jax.random.permutation(jax.random.fold_in(stream_key, 2), amount)]


def scatter_about(key, dims, scale, bound, split=(), held_as=jnp.bfloat16):
    gain = level_of(key, dims, split, -0.22, 0.18) if split else 1.0
    array = jax.random.normal(key, dims, jnp.float32) * scale * gain
    return jnp.minimum(jnp.maximum(array, -bound), bound).astype(held_as)


def setup_inputs(seed: int = 0) -> dict:
    splits = jax.random.split(jax.random.key(seed), 14)
    return {
        "hidden_in": scatter_about(splits[0], (ROWS, SEQ_LEN, D), 1.0, 6.0, ((0, 16), (1, 2))),
        "segment_ids": jax.vmap(lambda own: jnp.searchsorted(jnp.cumsum(ragged(own, SEGS, SEQ_LEN, SEG_MOST, 0)), jnp.arange(SEQ_LEN), side="right"))(jax.random.split(splits[1], ROWS)).reshape((ROWS, SEQ_LEN)).astype(jnp.int32),
        "qkv_weight": scatter_about(splits[2], (D, 3 * D), (D // 2) ** -0.5, 0.3125),
        "qv_bias": scatter_about(splits[3], (2, D), 1.0, 5.0, (), jnp.float32),
        "out_weight": scatter_about(splits[4], (D, D), (D // 4) ** -0.5, 0.4375),
        "out_bias": scatter_about(splits[5], (D,), 0.5, 3.0, (), jnp.float32),
        "norm_gain": jnp.clip(1.0 + 0.1 * jax.random.normal(splits[6], (2, D), jnp.float32), 0.5, 1.5),
        "norm_shift": scatter_about(splits[7], (2, D), 0.5, 3.0, (), jnp.float32),
        "ffn_in_weight": scatter_about(splits[8], (D, FF), D ** -0.5, 0.21875),
        "ffn_in_bias": scatter_about(splits[9], (FF,), 0.5, 3.0, (), jnp.float32),
        "ffn_out_weight": scatter_about(splits[10], (FF, D), (FF // 2) ** -0.5, 0.15625),
        "ffn_out_bias": scatter_about(splits[11], (D,), 0.5, 3.0, (), jnp.float32),
        "out_grad": scatter_about(splits[12], (ROWS, SEQ_LEN, D), 1.0, 6.0, ((0, 16), (1, 2))),
    }


epsilon = 1e-05
gelu_scale = 0.7978845608028654
masked_value = -1e+30
highest = lax.Precision.HIGHEST

@jax.custom_vjp
def low(v):
    return lax.optimization_barrier(v.astype(jnp.bfloat16)).astype(jnp.float32)

@jax.custom_vjp
def low_back(v):
    return v

def low_keep(v):
    return (low(v), None)

def low_pass(kept, grad):
    return (grad,)

def back_keep(v):
    return (v, None)

def back_low(kept, grad):
    return (low(grad),)
low.defvjp(low_keep, low_pass)
low_back.defvjp(back_keep, back_low)

def matmul(left, right):
    return jnp.dot(left, right, precision=highest)

def layer_norm(inputs, gain_row, shift_row):
    row_mean = lax.optimization_barrier(jnp.mean(inputs, axis=-1, keepdims=True))
    offset = inputs - row_mean
    spread = lax.optimization_barrier(jnp.mean(offset * offset, axis=-1, keepdims=True))
    return offset * lax.rsqrt(spread + epsilon) * gain_row + shift_row

def gelu_tanh(inputs):
    return 0.5 * inputs * (1.0 + jnp.tanh(gelu_scale * (inputs + 0.044715 * inputs * inputs * inputs)))

def one_layer(hidden_state, segment_rows, weights):
    weight_qkv, bias_qv, weight_out, bias_out, norm_gains, norm_shifts, weight_in, bias_in, weight_down, bias_down = weights
    row_count, length_all, model_width = hidden_state.shape
    head_count = model_width // HEAD_DIM
    score_scale = HEAD_DIM ** (-0.5)
    packed = matmul(low(hidden_state), weight_qkv)
    queries = low(low_back(packed[..., :model_width] + bias_qv[0])).reshape(row_count, length_all, head_count, HEAD_DIM)
    keys_all = low(low_back(packed[..., model_width:2 * model_width])).reshape(row_count, length_all, head_count, HEAD_DIM)
    values_all = low(low_back(packed[..., 2 * model_width:] + bias_qv[1])).reshape(row_count, length_all, head_count, HEAD_DIM)
    scores = low_back(jnp.einsum('rqhd,rkhd->rhqk', queries, keys_all, precision=highest) * score_scale)
    same_segment = (segment_rows[:, :, None] == segment_rows[:, None, :])[:, None]
    scores = jnp.where(same_segment, scores, masked_value)
    row_maximum = lax.optimization_barrier(jnp.max(scores, axis=-1, keepdims=True))
    exponents = jnp.exp(scores - row_maximum)
    softmax_low = low(exponents / lax.optimization_barrier(jnp.sum(exponents, axis=-1, keepdims=True)))
    attended = jnp.einsum('rhqk,rkhd->rqhd', softmax_low, values_all, precision=highest)
    attended = low(low_back(attended.reshape(row_count, length_all, model_width)))
    residual = hidden_state + low_back(matmul(attended, weight_out) + bias_out)
    normalized = layer_norm(residual, norm_gains[0], norm_shifts[0])
    ffn_inner = low_back(matmul(low(normalized), weight_in) + bias_in)
    activation = low(gelu_tanh(ffn_inner))
    residual_two = normalized + low_back(matmul(activation, weight_down) + bias_down)
    return layer_norm(residual_two, norm_gains[1], norm_shifts[1])

def reference(hidden_in, segment_ids, qkv_weight, qv_bias, out_weight, out_bias, norm_gain, norm_shift, ffn_in_weight, ffn_in_bias, ffn_out_weight, ffn_out_bias, out_grad):
    weights = tuple((weight_array.astype(jnp.float32) for weight_array in (qkv_weight, qv_bias, out_weight, out_bias, norm_gain, norm_shift, ffn_in_weight, ffn_in_bias, ffn_out_weight, ffn_out_bias)))
    total_rows = hidden_in.shape[0]
    group_rows = math.gcd(total_rows, max(1, 4096 // SEQ_LEN))
    block_count = total_rows // group_rows
    start_state = hidden_in.astype(jnp.float32).reshape(block_count, group_rows, SEQ_LEN, D)
    segment_blocks = segment_ids.reshape(block_count, group_rows, SEQ_LEN)
    cotangent = out_grad.astype(jnp.float32).reshape(block_count, group_rows, SEQ_LEN, D)

    def whole_net(first_state, layer_weights):

        def per_block(block_args):
            hidden_state, segment_rows = block_args
            for layer_index in range(LAYERS):
                hidden_state = one_layer(hidden_state, segment_rows, layer_weights)
            return hidden_state
        return lax.map(jax.checkpoint(per_block), (first_state, segment_blocks))
    final_state, pullback = jax.vjp(whole_net, start_state, weights)
    state_grad, weight_grads = pullback(cotangent)
    hidden_out = final_state.reshape(total_rows, SEQ_LEN, D).astype(jnp.bfloat16)
    input_grad = state_grad.reshape(total_rows, SEQ_LEN, D).astype(jnp.bfloat16)
    return (hidden_out, input_grad, weight_grads[0], weight_grads[1], weight_grads[2], weight_grads[3], weight_grads[4], weight_grads[5], weight_grads[6], weight_grads[7], weight_grads[8], weight_grads[9])
```

```python
import functools
import jax, jax.numpy as jnp
from jax import lax
from jax.experimental import pallas as pl
from jax.experimental.pallas import tpu as pltpu
from jax.sharding import PartitionSpec as P

bf16, f32 = jnp.bfloat16, jnp.float32
QB = 256
LANES = 128
BIG = 1e30
NT = (((1,), (1,)), ((), ()))


def dot(a, b):
    return lax.dot_general(a, b, (((1,), (0,)), ((), ())), preferred_element_type=f32)


def dot_nt(a, b):
    return lax.dot_general(a, b, NT, preferred_element_type=f32)


OTHER_LENGTHS = (0, 128, 256, 512)


def window_plan(own_segments, other_segments, half):
    n = own_segments.shape[0]
    blocks = n // QB
    first, last = own_segments[::QB], own_segments[QB - 1 :: QB]
    rows = []
    for b in range(blocks):
        overlap = (own_segments >= first[b]) & (own_segments <= last[b])
        outside = (jnp.arange(n) // QB) != b
        wide = jnp.any(overlap & outside)
        hit = (other_segments >= first[b]) & (other_segments <= last[b])
        count = jnp.sum(hit.astype(jnp.int32))
        code = sum((count > length).astype(jnp.int32) for length in OTHER_LENGTHS[:-1])
        rows.append(code * 2 + wide.astype(jnp.int32))
    return jnp.concatenate([jnp.stack(rows), jnp.reshape(half, (1,)).astype(jnp.int32)])


def query_features(segments):
    lane = jnp.arange(LANES) % 64
    other = (segments[:, None] != lane[None, :]) & (lane < 4)[None, :]
    return jnp.where(other, BIG, 0.0).astype(bf16)


def key_features(segments):
    lane = jnp.arange(LANES) % 64
    same = (segments[:, None] == lane[None, :]) & (lane < 4)[None, :]
    return jnp.where(same, -1.0, jnp.where((lane >= 4) & (lane < 7), 1.0, 0.0)[None, :]).astype(bf16)


def per_window(plan_ref, b, body):
    code = plan_ref[b]
    upper = plan_ref[2] == 1
    for c, length in enumerate(OTHER_LENGTHS):
        for wide in (0, 1):
            @pl.when(code == c * 2 + wide)
            def _(length=length, wide=wide):
                own_start = 0 if wide else pl.multiple_of(b * QB, QB)
                own_length = 2 * QB if wide else QB
                other_start = pl.multiple_of(jnp.where(upper, 2 * QB - length, 0), 128)
                body(own_start, own_length, other_start, length)


def forward_kernel(plan, q, k, v, ko, vo, qf, kf, kfo, out, lse, k2, v2):
    pair = pl.program_id(0)
    lane = lax.broadcasted_iota(jnp.int32, (1, LANES), 1)
    low = lane < 64
    n = k.shape[0]
    one = jnp.ones((1, LANES), bf16)
    for part, (kr, vr, fr) in enumerate(((k, v, kf), (ko, vo, kfo))):
        rows = pl.ds(part * n, n)
        kk, vv, ff = kr[...], vr[...], fr[...]
        k2[0, rows] = jnp.where(low, kk, ff)
        k2[1, rows] = jnp.where(low, ff, kk)
        v2[0, rows] = jnp.where(low, vv, one)
        v2[1, rows] = jnp.where(low, one, vv)

    @pl.when(pair == 0)
    def _():
        lse[...] = jnp.zeros_like(lse)

    @pl.loop(0, n // QB)
    def _(b):
        qrows = pl.ds(pl.multiple_of(b * QB, QB), QB)

        def body(own_start, own_length, other_start, other_length):
            qq, feature = q[qrows] * jnp.bfloat16(0.125), qf[qrows]
            results = []
            for h in range(2):
                queries = jnp.where(low, qq, feature) if h == 0 else jnp.where(low, feature, qq)
                own = pl.ds(own_start, own_length)
                s = [dot_nt(queries, k2[h, own])]
                if other_length:
                    other = pl.ds(n + other_start, other_length)
                    s.append(dot_nt(queries, k2[h, other]))
                top = functools.reduce(jnp.maximum, [jnp.max(x, axis=1, keepdims=True) for x in s])
                p = [jnp.exp(x - top).astype(bf16) for x in s]
                acc = dot(p[0], v2[h, own])
                if other_length:
                    acc = acc + dot(p[1], v2[h, other])
                results.append((top, acc))
            (top_a, acc_a), (top_b, acc_b) = results
            total = pltpu.roll(jnp.where(low, acc_b, acc_a), 64, 1)
            out[qrows] = (jnp.where(low, acc_a, acc_b) / total).astype(bf16)
            logs = jnp.where(low, top_a, top_b) + jnp.log(total)
            spread = jnp.where(lane == 2 * pair, logs[:, 0:1], jnp.where(lane == 2 * pair + 1, logs[:, 64:65], lse[qrows]))
            lse[qrows] = spread

        per_window(plan, b, body)


def attention_forward(plan, queries, kv, kv_other, qf, kf, kfo):
    n, width = queries.shape
    pairs = width // LANES
    block = lambda off: pl.BlockSpec((n, LANES), lambda p, *_: (0, off + p))
    fixed = pl.BlockSpec((n, LANES), lambda p, *_: (0, 0))
    return pl.pallas_call(
        forward_kernel,
        grid_spec=pltpu.PrefetchScalarGridSpec(
            num_scalar_prefetch=1,
            grid=(pairs,),
            in_specs=[block(0), block(0), block(pairs), block(0), block(pairs), fixed, fixed, fixed],
            out_specs=[block(0), fixed],
            scratch_shapes=[pltpu.VMEM((2, 2 * n, LANES), bf16), pltpu.VMEM((2, 2 * n, LANES), bf16)],
        ),
        out_shape=[jax.ShapeDtypeStruct((n, pairs * LANES), bf16), jax.ShapeDtypeStruct((n, LANES), f32)],
        compiler_params=pltpu.CompilerParams(vmem_limit_bytes=24 << 20),
        cost_estimate=pl.CostEstimate(flops=4 * n * 2 * n * pairs * LANES * 2, bytes_accessed=n * LANES * pairs * 14, transcendentals=n * 2 * n * pairs * 2),
        name="attention_forward",
    )(plan, queries, kv, kv, kv_other, kv_other, qf, kf, kfo)


def split3(x):
    hi = x.astype(bf16).astype(f32)
    mid = (x - hi).astype(bf16).astype(f32)
    return hi, mid, x - hi - mid


def backward_kernel(plan, q, k, v, ko, vo, do, o, lse, qf, kf, kfo, dq, dk, dv, dko, dvo, k2, v2, kt, q2, do2, dks, dvs):
    pair = pl.program_id(0)
    lane = lax.broadcasted_iota(jnp.int32, (1, LANES), 1)
    low = lane < 64
    n = k.shape[0]
    sub = lane % 64
    for part, (kr, vr, fr) in enumerate(((k, v, kf), (ko, vo, kfo))):
        rows = pl.ds(part * n, n)
        kk, vv, ff = kr[...], vr[...], fr[...]
        k2[0, rows] = jnp.where(low, kk, ff)
        k2[1, rows] = jnp.where(low, ff, kk)
        v2[0, rows] = jnp.where(low, vv, ff)
        v2[1, rows] = jnp.where(low, ff, vv)
        kt[:, rows] = kk.astype(f32).T.astype(bf16)
    qq = q[...] * jnp.bfloat16(0.125)
    feature = qf[...]
    dd = do[...]
    product = dd.astype(f32) * o[...].astype(f32)
    logs = lse[...]
    for h in range(2):
        mine = low if h == 0 else jnp.logical_not(low)
        head_lse = jnp.sum(jnp.where(lane == 2 * pair + h, logs, 0.0), axis=1, keepdims=True)
        delta = jnp.sum(jnp.where(mine, product, 0.0), axis=1, keepdims=True)
        a, b, c = split3(-head_lse)
        extra = jnp.where(sub == 4, a, jnp.where(sub == 5, b, jnp.where(sub == 6, c, feature.astype(f32)))).astype(bf16)
        q2[h] = jnp.where(mine, qq, extra)
        a, b, c = split3(-delta)
        extra = jnp.where(sub == 4, a, jnp.where(sub == 5, b, jnp.where(sub == 6, c, 0.0))).astype(bf16)
        do2[h] = jnp.where(mine, dd, extra)
    dks[...] = jnp.zeros_like(dks)
    dvs[...] = jnp.zeros_like(dvs)

    @pl.loop(0, n // QB)
    def _(b):
        qrows = pl.ds(pl.multiple_of(b * QB, QB), QB)

        def body(own_start, own_length, other_start, other_length):
            gradients = []
            d_pair = do[qrows]
            q_pair = q[qrows] * jnp.bfloat16(0.125)
            windows = [pl.ds(own_start, own_length)]
            if other_length:
                windows.append(pl.ds(n + other_start, other_length))
            total = [None, None]
            for win in windows:
                terms_v, terms_k = [], []
                for h in range(2):
                    queries, outward = q2[h, qrows], do2[h, qrows]
                    p = jnp.exp(dot_nt(k2[h, win], queries))
                    ds = (p * dot_nt(v2[h, win], outward)).astype(bf16)
                    terms_v.append(dot(p.astype(bf16), d_pair))
                    terms_k.append(dot(ds, q_pair))
                    part = dot(kt[h * 64 : h * 64 + 64, win], ds)
                    total[h] = part if total[h] is None else total[h] + part
                dvs[win] += jnp.where(low, terms_v[0], terms_v[1])
                dks[win] += jnp.where(low, terms_k[0], terms_k[1])
            both = jnp.concatenate(total, axis=0) * 0.125
            dq[qrows] = both.T.astype(bf16)

        per_window(plan, b, body)

    dk[...] = dks[0:n].astype(bf16)
    dv[...] = dvs[0:n].astype(bf16)
    dko[...] = dks[n : 2 * n].astype(bf16)
    dvo[...] = dvs[n : 2 * n].astype(bf16)


def attention_backward(plan, queries, kv, kv_other, d_out, out, lse, qf, kf, kfo):
    n, width = queries.shape
    pairs = width // LANES
    block = lambda off: pl.BlockSpec((n, LANES), lambda p, *_: (0, off + p))
    fixed = pl.BlockSpec((n, LANES), lambda p, *_: (0, 0))
    shape = jax.ShapeDtypeStruct((n, pairs * LANES), bf16)
    return pl.pallas_call(
        backward_kernel,
        grid_spec=pltpu.PrefetchScalarGridSpec(
            num_scalar_prefetch=1,
            grid=(pairs,),
            in_specs=[block(0), block(0), block(pairs), block(0), block(pairs), block(0), block(0), fixed, fixed, fixed, fixed],
            out_specs=[block(0)] * 5,
            scratch_shapes=[
                pltpu.VMEM((2, 2 * n, LANES), bf16),
                pltpu.VMEM((2, 2 * n, LANES), bf16),
                pltpu.VMEM((LANES, 2 * n), bf16),
                pltpu.VMEM((2, n, LANES), bf16),
                pltpu.VMEM((2, n, LANES), bf16),
                pltpu.VMEM((2 * n, LANES), f32),
                pltpu.VMEM((2 * n, LANES), f32),
            ],
        ),
        out_shape=[shape] * 5,
        compiler_params=pltpu.CompilerParams(vmem_limit_bytes=32 << 20),
        cost_estimate=pl.CostEstimate(flops=10 * n * 2 * n * pairs * LANES * 2, bytes_accessed=n * LANES * pairs * 24, transcendentals=n * 2 * n * pairs * 2),
        name="attention_backward",
    )(plan, queries, kv, kv, kv_other, kv_other, d_out, out, lse, qf, kf, kfo)


LAYERS = 2
EPSILON = 1e-05
GELU_SCALE = 0.7978845608028654
GELU_CUBIC = 0.044715
AXES = ("batch", "seq")
SEQ_BIT, CORE_BIT = 0, 1


def norm_forward(v, gain, shift):
    offset = v - jnp.mean(v, axis=-1, keepdims=True)
    root = lax.rsqrt(jnp.mean(offset * offset, axis=-1, keepdims=True) + EPSILON)
    n = offset * root
    return n * gain + shift, n, root


def norm_backward(g, n, root, gain):
    dn = g * gain
    back = root * (dn - jnp.mean(dn, axis=-1, keepdims=True) - n * jnp.mean(dn * n, axis=-1, keepdims=True))
    return back, jnp.sum(g * n, axis=0), jnp.sum(g, axis=0)


def gelu_parts(v):
    t = jnp.tanh(GELU_SCALE * (v + GELU_CUBIC * v * v * v))
    return t


def gelu(v):
    return 0.5 * v * (1.0 + gelu_parts(v))


def gelu_slope(v):
    t = gelu_parts(v)
    return 0.5 * (1.0 + t) + 0.5 * v * (1.0 - t * t) * GELU_SCALE * (1.0 + 3.0 * GELU_CUBIC * v * v)


def tn(a, b):
    return lax.dot_general(a, b, (((0,), (0,)), ((), ())), preferred_element_type=f32)


def token_sum(v):
    return jnp.sum(v.astype(f32), axis=0)


class Wires:
    def __init__(self):
        self.count = lax.axis_size(AXES)
        self.place = lax.axis_index(AXES)
        self.bits = self.count.bit_length() - 1

    def bit(self, b):
        return (self.place >> b) & 1

    def exchange(self, x, b):
        return lax.ppermute(x, AXES, [(i, i ^ (1 << b)) for i in range(self.count)])

    def swap(self, x):
        pairs = [(i, i ^ 3) for i in range(self.count) if i % 4 in (1, 2)]
        moved = lax.ppermute(x, AXES, pairs)
        stays = self.bit(0) == self.bit(1)
        return jnp.where(stays, x, moved)

    def scatter(self, piece, order):
        for b in order:
            half = piece.shape[0] // 2
            keep = lax.dynamic_slice_in_dim(piece, self.bit(b) * half, half, 0)
            send = lax.dynamic_slice_in_dim(piece, (1 - self.bit(b)) * half, half, 0)
            piece = (keep.astype(f32) + self.exchange(send, b).astype(f32)).astype(bf16)
        return piece

    def gather(self, piece, order):
        for b in reversed(order):
            other = self.exchange(piece, b)
            first = self.bit(b) == 0
            piece = jnp.concatenate([jnp.where(first, piece, other), jnp.where(first, other, piece)], axis=0)
        return piece

    def orders(self):
        rest = list(range(2, self.bits))
        if not rest:
            return [[0], [0]]
        return [[0] + rest, rest[:1] + [0] + rest[1:]]


def weight_terms(wires, left, right):
    half = left.shape[1] // 2
    mine = lax.dynamic_slice_in_dim(left, wires.bit(CORE_BIT) * half, half, 1)
    theirs = lax.dynamic_slice_in_dim(left, (1 - wires.bit(CORE_BIT)) * half, half, 1)
    columns = right.shape[1] // 2
    return [(tn(mine, part), tn(theirs, part)) for part in (right[:, :columns], right[:, columns:])]


def add_terms(first, second):
    if first is None:
        return second
    return [tuple(a + b for a, b in zip(x, y)) for x, y in zip(first, second)]


def reduce_weight(wires, terms):
    out = []
    for (mine, theirs), order in zip(terms, wires.orders()):
        arrived = wires.exchange(theirs.astype(bf16), CORE_BIT)
        piece = (mine + arrived.astype(f32)).astype(bf16)
        piece = wires.scatter(piece, order)
        out.append(wires.gather(piece, [CORE_BIT] + order))
    return jnp.concatenate(out, axis=1).astype(f32)


def layer_forward(x, places, wires, weights):
    w_qkv, b_qv, w_out, b_out, gains, shifts, w_in, b_in, w_down, b_down = weights
    plan, qf, kf, kfo = places
    width = x.shape[-1]
    x_low = x.astype(bf16)
    bias = jnp.concatenate([jnp.zeros_like(b_qv[1]), b_qv[1]])
    kv = (jnp.dot(x_low, w_qkv[:, width:], preferred_element_type=f32) + bias).astype(bf16)
    kv_other = wires.exchange(kv, CORE_BIT)
    q = (jnp.dot(x_low, w_qkv[:, :width], preferred_element_type=f32) + b_qv[0]).astype(bf16)
    attended, lse = attention_forward(plan, q, kv, kv_other, qf, kf, kfo)
    residual = x + jnp.dot(attended, w_out, preferred_element_type=f32) + b_out
    normalized, n1, r1 = norm_forward(residual, gains[0], shifts[0])
    normalized_low = normalized.astype(bf16)
    inner = jnp.dot(normalized_low, w_in, preferred_element_type=f32) + b_in
    activation = gelu(inner).astype(bf16)
    residual_two = normalized + jnp.dot(activation, w_down, preferred_element_type=f32) + b_down
    out, n2, r2 = norm_forward(residual_two, gains[1], shifts[1])
    return out, (x_low, q, kv, kv_other, attended, lse, n1, r1, normalized_low, inner, activation, n2, r2)


def layer_backward(g, kept, places, wires, weights):
    w_qkv, b_qv, w_out, b_out, gains, shifts, w_in, b_in, w_down, b_down = weights
    plan, qf, kf, kfo = places
    x_low, q, kv, kv_other, attended, lse, n1, r1, normalized_low, inner, activation, n2, r2 = kept
    width = g.shape[-1]
    g_two, gain_two, shift_two = norm_backward(g, n2, r2, gains[1])
    branch_two = g_two.astype(bf16)
    d_down = weight_terms(wires, activation, branch_two)
    d_b_down = token_sum(branch_two)
    d_act = lax.dot_general(branch_two, w_down, NT, preferred_element_type=f32)
    d_inner = (gelu_slope(inner) * d_act).astype(bf16)
    d_b_in = token_sum(d_inner)
    d_in = weight_terms(wires, normalized_low, d_inner)
    g_norm = g_two + lax.dot_general(d_inner, w_in, NT, preferred_element_type=f32)
    g_res, gain_one, shift_one = norm_backward(g_norm, n1, r1, gains[0])
    branch = g_res.astype(bf16)
    d_b_out = token_sum(branch)
    d_out = weight_terms(wires, attended, branch)
    d_attended = lax.dot_general(branch, w_out, NT, preferred_element_type=f32).astype(bf16)
    dq, dk, dv, dko, dvo = attention_backward(plan, q, kv, kv_other, d_attended, attended, lse, qf, kf, kfo)
    arrived_k, arrived_v = wires.exchange(dko, CORE_BIT), wires.exchange(dvo, CORE_BIT)
    dk = (dk.astype(f32) + arrived_k.astype(f32)).astype(bf16)
    dv = (dv.astype(f32) + arrived_v.astype(f32)).astype(bf16)
    packed = jnp.concatenate([dq, dk, dv], axis=-1)
    d_qkv = weight_terms(wires, x_low, packed)
    g = g_res + lax.dot_general(packed, w_qkv, NT, preferred_element_type=f32)
    small = jnp.concatenate([token_sum(dq), token_sum(dv), d_b_out, gain_one, gain_two, shift_one, shift_two, d_b_in, d_b_down])
    return g, (d_down, d_in, d_out, d_qkv), small


def per_device(hidden_in, segment_ids, w_qkv, b_qv, w_out, b_out, gains, shifts, w_in, b_in, w_down, b_down, out_grad):
    weights = (w_qkv, b_qv, w_out, b_out, gains, shifts, w_in, b_in, w_down, b_down)
    wires = Wires()
    width = hidden_in.shape[-1]
    start = wires.swap(hidden_in[0])
    segments = wires.swap(segment_ids[0])
    g_last = wires.swap(out_grad[0])
    n = start.shape[0]
    core = wires.bit(CORE_BIT)
    own = lax.dynamic_slice_in_dim(segments, core * n, n, 0)
    other = lax.dynamic_slice_in_dim(segments, (1 - core) * n, n, 0)
    places = (window_plan(own, other, core), query_features(own), key_features(own), key_features(other))
    x = start.astype(f32)
    kept = []
    for _ in range(LAYERS):
        x, saved = layer_forward(x, places, wires, weights)
        kept.append(saved)
    hidden_out = wires.swap(x.astype(bf16))
    g = g_last.astype(f32)
    terms, small = [None] * 4, 0.0
    for saved in reversed(kept):
        g, new_terms, new_small = layer_backward(g, saved, places, wires, weights)
        terms = [add_terms(a, b) for a, b in zip(terms, new_terms)]
        small = small + new_small
    for b in range(wires.bits):
        small = small + wires.exchange(small, b)
    d_down, d_in, d_out, d_qkv = [reduce_weight(wires, t) for t in terms]
    input_grad = wires.swap(g.astype(bf16))
    ff = w_in.shape[1]
    rows = jnp.split(small, [2 * width, 3 * width, 5 * width, 7 * width, 7 * width + ff])
    return (
        hidden_out[None],
        input_grad[None],
        d_qkv,
        rows[0].reshape(2, width),
        d_out,
        rows[1],
        rows[2].reshape(2, width),
        rows[3].reshape(2, width),
        d_in,
        rows[4],
        d_down,
        rows[5],
    )


def solution(mesh):
    tokens, copied = P("batch", "seq", None), P()
    return jax.shard_map(
        per_device,
        mesh=mesh,
        in_specs=(tokens, P("batch", None)) + (copied,) * 10 + (tokens,),
        out_specs=(tokens, tokens) + (copied,) * 10,
        check_vma=False,
    )
```
